256 devices in a mesh: tok: 32 (over x, z), head: 8 (over y, core).
Axes of the slice: x: 4, y: 4, z: 8, core: 2. Of those that a mesh axis runs over, the one named last changes fastest.
Arguments:
- queries: bfloat16 [12288, 4096], P('tok', 'head'), may hold values from -100 to 100
- keys: bfloat16 [12288, 1024], P('tok', 'head'), may hold values from -5 to 5
- values: bfloat16 [12288, 1024], P('tok', 'head'), may hold values from -6 to 6
- lengths: int32 [16], replicated, may hold values from 1 to 6144, 12288 in all
- out_weight: bfloat16 [4096, 4096], P('head', 'tok'), may hold values from -0.09375 to 0.09375
Outputs:
- mixed: bfloat16 [12288, 4096], P('tok', 'head')
The draws below stay inside these ranges and needn't reach their ends.
Inputs may be any that keep to these rules, and one draw needn't show every extreme that they name: Every document has at most 6144 tokens and the lengths sum to 12288.
All inputs are finite; a program needn't handle non-finite values.
Results may differ from the reference program's by a relative error of at most 0.015.
Values may be sent and summed in bfloat16 or wider, within the bound.
A program may use at most 64 MiB of HBM per device.

```python
import math
import jax
import jax.numpy as jnp
import numpy as np
from jax import lax

D = 4096
QH = 32
KVH = 8
HD = 128
DOCS = 16
TOKENS = 12288
MOST = 6144


def shared_keys(key):
    base = jax.random.normal(jax.random.fold_in(key, 7), (TOKENS, KVH * HD), jnp.float32)
    base = jnp.clip(base, -5.0, 5.0)
    return base


def draw_keys(key, part):
    return shared_keys(key).astype(jnp.bfloat16)


def draw_queries(key, part):
    fresh = jax.random.normal(jax.random.fold_in(key, 11), (TOKENS, QH * HD), jnp.float32)
    fresh = jnp.clip(fresh, -6.0, 6.0)
    return fresh.astype(jnp.bfloat16)


def levels(rng, extent, pieces, low, top_value):
    factor_of, own = 1.0, jax.random.fold_in(rng, 6)
    for dim, shards_of in pieces:
        heights = jnp.exp(jax.random.uniform(jax.random.fold_in(own, dim), (shards_of,), jnp.float32, low / len(pieces), top_value / len(pieces)))
        factor_of = factor_of * jnp.repeat(heights, extent[dim] // shards_of).reshape([-1 if axis == dim else 1 for axis in range(len(extent))])
    return factor_of


def length_profile(count, total, reach, lean):
    portions = [(1 << 20) // math.isqrt(grade ** lean) + 1 for grade in range(2, count + 1)]
    rest, given = total - reach - (count - 1), [1] * (count - 1)
    while rest > 0:
        movable = [i for i in range(count - 1) if given[i] < reach]
        pool, budget = sum([portions[i] for i in movable]), rest
        for i in movable:
            more = min(reach - given[i], max(1, budget * portions[i] // pool), rest)
            given[i] = given[i] + more
            rest = rest - more
    return np.array([reach] + given)


def uneven(stream_key, amount, total, bound, skew):
    if amount == 2:
        one = jax.random.randint(stream_key, (), max(1, total - bound), min(bound, total - 1) + 1)
        return jnp.stack([one, total - one])
    sizes = jnp.asarray(length_profile(amount, total, bound, skew), jnp.int32)
    couples = (amount - 1) // 2
    donor, taker = sizes[1:1 + 2 * couples:2], sizes[2:2 + 2 * couples:2]
    room = jnp.minimum(donor - 1, bound - taker)
    moved = jax.random.randint(jax.random.fold_in(stream_key, 1), (couples,), 0, 1 << 20) % (room + 1)
    sizes = sizes.at[1:1 + 2 * couples:2].set(donor - moved).at[2:2 + 2 * couples:2].set(taker + moved)
    return sizes[jax.random.permutation(jax.random.fold_in(stream_key, 2), amount)]


def bell_draw(own_key, extent, scale, most, cuts=(), kind=jnp.bfloat16):
    drawn = scale * jax.random.normal(own_key, extent, jnp.float32)
    if cuts:
        drawn = drawn * levels(own_key, extent, cuts, -0.22, 0.18)
    return jnp.clip(drawn, -most, most).astype(kind)


def setup_inputs(seed: int = 0) -> dict:
    splits = jax.random.split(jax.random.key(seed), 6)
    return {
        "queries": draw_queries(jax.random.fold_in(splits[5], 71), 0),
        "keys": draw_keys(jax.random.fold_in(splits[5], 71), 0),
        "values": bell_draw(splits[2], (TOKENS, KVH * HD), 1.0, 6.0, ((0, 32), (1, 8))),
        "lengths": uneven(splits[3], DOCS, TOKENS, MOST, 2).astype(jnp.int32),
        "out_weight": bell_draw(splits[4], (QH * HD, D), (QH * HD) ** -0.5, 0.09375, ((0, 8), (1, 32))),
    }


def doc_index(lengths, positions):
    ends = jnp.cumsum(lengths)
    return jnp.sum((positions[:, None] >= ends[None, :]).astype(jnp.int32), axis=1).astype(jnp.int32)


def reference(queries, keys, values, lengths, out_weight):
    ratio = QH // KVH
    block = min(512, TOKENS)
    nblocks = TOKENS // block
    scale = 1.0 / (HD ** 0.5)
    positions = jnp.arange(TOKENS, dtype=jnp.int32)
    docs = doc_index(lengths, positions)
    qall = queries.reshape(TOKENS, KVH, ratio, HD)
    kall = keys.reshape(TOKENS, KVH, HD)
    vall = values.reshape(TOKENS, KVH, HD)

    def one_block(index):
        group = index // nblocks
        start = (index % nblocks) * block
        qblock = lax.dynamic_slice_in_dim(qall, start, block, 0)
        qblock = lax.dynamic_index_in_dim(qblock, group, 1, keepdims=False)
        kgroup = lax.dynamic_index_in_dim(kall, group, 1, keepdims=False)
        vgroup = lax.dynamic_index_in_dim(vall, group, 1, keepdims=False)
        scores = jnp.einsum("qrd,kd->rqk", qblock.astype(jnp.float32), kgroup.astype(jnp.float32)) * scale
        qpos = start + jnp.arange(block, dtype=jnp.int32)
        qdoc = lax.dynamic_slice_in_dim(docs, start, block, 0)
        allowed = (qdoc[:, None] == docs[None, :]) & (positions[None, :] <= qpos[:, None])
        scores = jnp.where(allowed[None], scores, jnp.float32(-1e30))
        top = jnp.max(scores, axis=-1, keepdims=True)
        weights = jnp.where(allowed[None], jnp.exp(scores - top), jnp.float32(0.0))
        total = jnp.sum(weights, axis=-1)
        low = weights.astype(jnp.bfloat16)
        summed = jnp.einsum("rqk,kd->rqd", low.astype(jnp.float32), vgroup.astype(jnp.float32))
        result = summed / total[..., None]
        return jnp.transpose(result, (1, 0, 2))

    outs = lax.map(one_block, jnp.arange(KVH * nblocks, dtype=jnp.int32))
    outs = outs.reshape(KVH, nblocks, block, ratio, HD)
    outs = jnp.transpose(outs, (1, 2, 0, 3, 4)).reshape(TOKENS, QH * HD)
    attn = outs.astype(jnp.bfloat16)
    return jnp.dot(attn, out_weight, preferred_element_type=jnp.float32).astype(jnp.bfloat16)
```

```python
import functools
import math

import jax
import jax.numpy as jnp
from jax import lax
from jax.experimental import pallas as pl
from jax.experimental.pallas import tpu as pltpu
from jax.sharding import PartitionSpec as P

HD = 128
NX, NZ, NY = 4, 8, 4
MESH = pl.DeviceIdType.MESH
FAR = -1e30
BF = jnp.bfloat16
F32 = jnp.float32


def kernel(
    scale,
    q_hbm, k_hbm, v_hbm, w_hbm, len_ref, o_ref,
    q, kv, wa, wb, start, top, total, accum, attn, mid, give, take, up, down, rup, rdown, tup, tdown,
    load, kv_recv, zp, zm, xs,
    axs, axr, azps, azpr, azms, azmr, bzps, bzpr, bzms, bzmr, bxs, bxr,
    gs, gr, rs, rr,
):
    tok = lax.axis_index("tok")
    head = lax.axis_index("head")
    x, z = lax.div(tok, NZ), lax.rem(tok, NZ)
    y, core = lax.div(head, 2), lax.rem(head, 2)
    rows = q.shape[0]
    ratio = q.shape[1] // HD
    ha = wa.shape[2]

    def at_xz(xx, zz):
        return {"tok": lax.rem(xx + NX, NX) * NZ + lax.rem(zz + NZ, NZ), "head": head}

    def at_y(yy, cc):
        return {"tok": tok, "head": lax.rem(yy + NY, NY) * 2 + cc}

    def remote(src, dst, send, recv, dev):
        return pltpu.make_async_remote_copy(
            src_ref=src, dst_ref=dst, send_sem=send, recv_sem=recv,
            device_id=dev, device_id_type=MESH,
        )

    east, west, south = at_xz(x + 1, z), at_xz(x + 3, z), at_xz(x + 2, z)
    zup, zdown = at_xz(x, z + 1), at_xz(x, z + 7)
    pair = at_y(y, 1 - core)
    yup, ydown = at_y(y + 1, core), at_y(y + 3, core)

    loads = [
        pltpu.make_async_copy(k_hbm, kv.at[0, z, 0], load.at[0]),
        pltpu.make_async_copy(v_hbm, kv.at[0, z, 1], load.at[1]),
        pltpu.make_async_copy(w_hbm.at[pl.ds(0, ha)], wa.at[z, x], load.at[2]),
        pltpu.make_async_copy(w_hbm.at[pl.ds(ha, wb.shape[2])], wb.at[x, z], load.at[3]),
        pltpu.make_async_copy(q_hbm, q, load.at[4]),
    ]
    for c in loads:
        c.start()

    barrier = pltpu.get_barrier_semaphore()
    greeted = (east, west, south, zup, zdown, pair, yup, ydown)
    for dev in greeted:
        pl.semaphore_signal(barrier, inc=1, device_id=dev, device_id_type=MESH)
    pl.semaphore_wait(barrier, len(greeted))

    def kv_zup(zz):
        return remote(kv.at[0, zz], kv.at[0, zz], zp.at[zz], kv_recv.at[0, zz], zup)

    def kv_zdown(zz):
        return remote(kv.at[1, zz], kv.at[1, zz], zm.at[zz], kv_recv.at[1, zz], zdown)

    def kv_east(t, zz, k):
        return remote(kv.at[t, zz], kv.at[t + 1, zz], xs.at[k], kv_recv.at[t + 1, zz], east)

    def kv_arrive(t, zz):
        remote(kv.at[t, zz], kv.at[t, zz], zp.at[0], kv_recv.at[t, zz], east).wait_recv()

    def item(k):
        na, nb = z + 1, NZ - z
        m = jnp.minimum(na, nb)
        both = k < 2 * m
        kind = jnp.where(both, lax.rem(k, 2), jnp.where(na > nb, 0, 1))
        j = jnp.where(both, lax.div(k, 2), k - m)
        return kind, jnp.where(kind == 0, z - j, z + j)

    def ax(d):
        return remote(wa.at[z, x], wa.at[z, x], axs.at[d - 1], axr.at[d - 1], at_xz(x + d, z))

    def azp(s):
        b = wa.at[lax.rem(z + NZ - s, NZ)]
        return remote(b, b, azps.at[s], azpr.at[s], zup)

    def azm(s):
        b = wa.at[lax.rem(z + s, NZ)]
        return remote(b, b, azms.at[s], azmr.at[s], zdown)

    def bzp(s):
        b = wb.at[x, lax.rem(z + NZ - s, NZ)]
        return remote(b, b, bzps.at[s], bzpr.at[s], zup)

    def bzm(s):
        b = wb.at[x, lax.rem(z + s, NZ)]
        return remote(b, b, bzms.at[s], bzmr.at[s], zdown)

    def bx(s):
        b = wb.at[lax.rem(x + s, NX)]
        return remote(b, b, bxs.at[s], bxr.at[s], west)

    last_up, last_down = lax.rem(z + 1, NZ) < 4, lax.rem(z + 7, NZ) >= 4
    get_up, get_down = z < 4, z >= 4

    loads[0].wait()
    loads[1].wait()

    @pl.when(z < NZ - 1)
    def _():
        kv_zup(z).start()

    @pl.when(x < NX - 1)
    def _():
        kv_east(0, z, 0).start()

    loads[2].wait()
    loads[3].wait()
    for d in (1, 2, 3):
        ax(d).start()
    bzp(0).start()
    bzm(0).start()
    loads[4].wait()

    qpos = tok * rows + lax.broadcasted_iota(jnp.int32, (rows, HD), 0)
    edge = jnp.int32(0)
    first = jnp.zeros((rows, HD), jnp.int32)
    for d in range(len_ref.shape[0]):
        edge = edge + len_ref[d]
        first = jnp.maximum(first, jnp.where(qpos >= edge, edge, 0))
    start[...] = first

    lane = lax.broadcasted_iota(jnp.int32, (rows, HD), 1)
    tiles = rows // HD

    def attend(t, zz, fresh):
        base = ((x - t) * NZ + zz) * rows
        kblock = kv[t, zz, 0]
        vblock = kv[t, zz, 1]
        near = start[...] - base
        allowed = []
        for j in range(tiles):
            ok = lane + j * HD >= near
            if fresh:
                ok = ok & (lane + j * HD <= lax.broadcasted_iota(jnp.int32, (rows, HD), 0))
            allowed.append(ok)
        for r in range(ratio):
            s = lax.dot_general(
                q[:, r * HD : (r + 1) * HD], kblock, (((1,), (1,)), ((), ())),
                preferred_element_type=F32,
            )
            parts = [
                jnp.where(allowed[j], s[:, j * HD : (j + 1) * HD], FAR) for j in range(tiles)
            ]
            peak = jnp.max(functools.reduce(jnp.maximum, parts), axis=1, keepdims=True)
            if fresh:
                new = jnp.broadcast_to(peak, (rows, HD))
            else:
                old = top[r]
                new = jnp.maximum(old, peak)
                fade = jnp.exp2((old - new) * scale)
            weights = [jnp.exp2((p - new) * scale) for p in parts]
            added = functools.reduce(jnp.add, weights)
            low = jnp.concatenate([w.astype(BF) for w in weights], axis=1)
            gain = jnp.dot(low, vblock, preferred_element_type=F32)
            top[r] = new
            if fresh:
                total[r] = added
                accum[r] = gain
            else:
                total[r] = total[r] * fade + added
                accum[r] = accum[r] * fade + gain

    attend(0, z, True)

    def step(k, carry):
        have_a = k <= z
        have_b = (x > 0) & (z + k - 1 < NZ)
        az, bz = z - k, z + k - 1

        @pl.when(have_a)
        def _():
            kv_arrive(0, az)

        @pl.when(have_a & (z < NZ - 1))
        def _():
            kv_zup(az).start()

        @pl.when(have_b)
        def _():
            kv_arrive(1, bz)

        @pl.when(have_b & (z > 0))
        def _():
            kv_zdown(bz).start()

        kind, zz = item(k)

        @pl.when((k <= NZ) & (x < NX - 1) & ((kind == 0) | (x > 0)))
        def _():
            kv_east(kind, zz, k).start()

        @pl.when(k == 1)
        def _():
            bzp(0).wait_recv()
            bzp(1).start()
            bzm(0).wait_recv()
            bzm(1).start()
            for d in (1, 2, 3):
                ax(d).wait_recv()
            azp(0).start()
            azm(0).start()

        @pl.when(k == 2)
        def _():
            bzp(1).wait_recv()
            bzp(2).start()
            bzm(1).wait_recv()
            bzm(2).start()

        @pl.when(k == 3)
        def _():
            bzp(2).wait_recv()
            bzm(2).wait_recv()
            azp(0).wait_recv()
            azp(1).start()
            azm(0).wait_recv()
            azm(1).start()

        @pl.when((k == 3) & last_up)
        def _():
            bzp(3).start()

        @pl.when((k == 3) & last_down)
        def _():
            bzm(3).start()

        @pl.when((k == 4) & get_up)
        def _():
            bzp(3).wait_recv()

        @pl.when((k == 4) & get_down)
        def _():
            bzm(3).wait_recv()

        @pl.when(k == 4)
        def _():
            bx(0).start()

        @pl.when(k == 5)
        def _():
            azp(1).wait_recv()
            azp(2).start()
            azm(1).wait_recv()
            azm(2).start()

        @pl.when(k == 7)
        def _():
            azp(2).wait_recv()
            azm(2).wait_recv()
            bx(0).wait_recv()
            bx(1).start()

        @pl.when((k == 7) & last_up)
        def _():
            azp(3).start()

        @pl.when((k == 7) & last_down)
        def _():
            azm(3).start()

        @pl.when(k == 9)
        def _():
            bx(1).wait_recv()
            bx(2).start()

        @pl.when(have_a)
        def _():
            attend(0, az, False)

        @pl.when(have_b)
        def _():
            attend(1, bz, False)

        kind, zz = item(k - 1)
        have_x = (k > 1) & (x > 0) & ((kind == 0) | (x > 1))

        @pl.when(have_x)
        def _():
            kv_arrive(kind + 1, zz)
            attend(kind + 1, zz, False)

        return carry

    lax.fori_loop(1, NZ + 2, step, 0)

    for r in range(ratio):
        whole = jnp.sum(total[r], axis=1, keepdims=True)
        attn[:, r * HD : (r + 1) * HD] = (accum[r] / whole).astype(BF)

    bx(2).wait_recv()

    @pl.when(get_up)
    def _():
        azp(3).wait_recv()

    @pl.when(get_down)
    def _():
        azm(3).wait_recv()

    def project(g, c):
        out = []
        for h in (0, 2):
            zz = c * 4 + h
            ra = jnp.concatenate([wa[zz, g], wa[zz + 1, g]], axis=1)
            rb = jnp.concatenate([wb[g, zz], wb[g, zz + 1]], axis=1)
            out.append(
                jnp.dot(attn[:, :ha], ra, preferred_element_type=F32)
                + jnp.dot(attn[:, ha:], rb, preferred_element_type=F32)
            )
        return jnp.concatenate(out, axis=1)

    def swap(i):
        return remote(give.at[i], take.at[i], gs.at[i], gr.at[i], pair)

    half = rows // 2
    lo, hi = pl.ds(0, half), pl.ds(half, half)
    targets = [lax.rem(y + d, NY) for d in (2, 1, 3, 0)]

    def first_pass(i, carry):
        g = lax.rem(y + jnp.where(i == 0, 2, jnp.where(i == 1, 1, jnp.where(i == 2, 3, 0))), NY)
        give[i] = project(g, 1 - core).astype(BF)
        swap(i).start()
        return carry

    lax.fori_loop(0, NY, first_pass, 0)

    far_up = remote(mid.at[lo], rup, rs.at[0], rr.at[0], yup)
    far_down = remote(mid.at[hi], rdown, rs.at[1], rr.at[1], ydown)
    up_hi = remote(up.at[hi], tup.at[hi], rs.at[2], rr.at[2], yup)
    down_lo = remote(down.at[lo], tdown.at[lo], rs.at[3], rr.at[3], ydown)
    up_lo = remote(up.at[lo], tup.at[lo], rs.at[4], rr.at[4], yup)
    down_hi = remote(down.at[hi], tdown.at[hi], rs.at[5], rr.at[5], ydown)

    def both_cores(i):
        mine = project(targets[i], core)
        swap(i).wait_recv()
        return mine + take[i].astype(F32)

    mid[...] = both_cores(0).astype(BF)
    far_up.start()
    far_down.start()
    part = both_cores(1)
    up[hi] = part[half:].astype(BF)
    accum_up = part[:half]
    up_hi.start()
    part = both_cores(2)
    down[lo] = part[:half].astype(BF)
    accum_down = part[half:]
    down_lo.start()
    far_up.wait_recv()
    up[lo] = (accum_up + rup[...].astype(F32)).astype(BF)
    up_lo.start()
    far_down.wait_recv()
    down[hi] = (accum_down + rdown[...].astype(F32)).astype(BF)
    down_hi.start()
    mine = both_cores(3)
    up_hi.wait_recv()
    down_lo.wait_recv()
    up_lo.wait_recv()
    down_hi.wait_recv()
    o_ref[...] = (mine + tup[...].astype(F32) + tdown[...].astype(F32)).astype(BF)

    for i in range(NY):
        swap(i).wait_send()
    for c in (far_up, far_down, up_hi, down_lo, up_lo, down_hi):
        c.wait_send()
    for d in (1, 2, 3):
        ax(d).wait_send()
    for s in range(3):
        for c in (azp(s), azm(s), bzp(s), bzm(s), bx(s)):
            c.wait_send()

    @pl.when(last_up)
    def _():
        azp(3).wait_send()
        bzp(3).wait_send()

    @pl.when(last_down)
    def _():
        azm(3).wait_send()
        bzm(3).wait_send()

    def drain(k, carry):
        @pl.when((k <= z) & (z < NZ - 1))
        def _():
            kv_zup(k).wait_send()

        @pl.when((k >= z) & (z > 0) & (x > 0) & (k < NZ))
        def _():
            kv_zdown(k).wait_send()

        kind, zz = item(k)

        @pl.when((x < NX - 1) & ((kind == 0) | (x > 0)))
        def _():
            kv_east(kind, zz, k).wait_send()

        return carry

    lax.fori_loop(0, NZ + 1, drain, 0)


def body(queries, keys, values, lengths, out_weight):
    rows, width = queries.shape
    depth = out_weight.shape[0]
    ha = depth // 2
    scale = math.log2(math.e) / math.sqrt(HD)
    ratio = width // HD
    dma = pltpu.SemaphoreType.DMA
    any_ = pl.BlockSpec(memory_space=pl.ANY)
    return pl.pallas_call(
        functools.partial(kernel, scale),
        out_shape=jax.ShapeDtypeStruct((rows, width), BF),
        in_specs=[any_, any_, any_, any_, pl.BlockSpec(memory_space=pltpu.SMEM)],
        out_specs=pl.BlockSpec(memory_space=pltpu.VMEM),
        scratch_shapes=[
            pltpu.VMEM((rows, width), BF),
            pltpu.VMEM((3, NZ, 2, rows, HD), BF),
            pltpu.VMEM((NZ, NX, ha, HD), BF),
            pltpu.VMEM((NX, NZ, depth - ha, HD), BF),
            pltpu.VMEM((rows, HD), jnp.int32),
            pltpu.VMEM((ratio, rows, HD), F32),
            pltpu.VMEM((ratio, rows, HD), F32),
            pltpu.VMEM((ratio, rows, HD), F32),
            pltpu.VMEM((rows, width), BF),
            pltpu.VMEM((rows, width), BF),
            pltpu.VMEM((NY, rows, width), BF),
            pltpu.VMEM((NY, rows, width), BF),
            pltpu.VMEM((rows, width), BF),
            pltpu.VMEM((rows, width), BF),
            pltpu.VMEM((rows // 2, width), BF),
            pltpu.VMEM((rows // 2, width), BF),
            pltpu.VMEM((rows, width), BF),
            pltpu.VMEM((rows, width), BF),
            dma((5,)), dma((3, NZ)), dma((NZ,)), dma((NZ,)), dma((NZ + 1,)),
            dma((3,)), dma((3,)),
            dma((4,)), dma((4,)), dma((4,)), dma((4,)),
            dma((4,)), dma((4,)), dma((4,)), dma((4,)),
            dma((3,)), dma((3,)),
            dma((NY,)), dma((NY,)), dma((6,)), dma((6,)),
        ],
        compiler_params=pltpu.CompilerParams(
            collective_id=0, has_side_effects=True, vmem_limit_bytes=60 * 1024 * 1024
        ),
    )(queries, keys, values, out_weight, lengths)


def solution(mesh):
    placed = (P("tok", "head"), P("tok", "head"), P("tok", "head"), P(), P("head", "tok"))
    return jax.shard_map(
        body, mesh=mesh, in_specs=placed, out_specs=P("tok", "head"), check_vma=False
    )
```

```python
import functools
import math

import jax
import jax.numpy as jnp
from jax import lax
from jax.experimental import pallas as pl
from jax.experimental.pallas import tpu as pltpu
from jax.sharding import PartitionSpec as P

HD = 128
NX, NZ, NY = 4, 8, 4
MESH = pl.DeviceIdType.MESH
FAR = -1e30
BF = jnp.bfloat16
F32 = jnp.float32
PLAN = {
    1: ((0, 1), (2, 0, 1), (2, 0, 2)),
    2: ((0, 2), (2, 0, 3), (2, 0, 4), (2, 1, 0)),
    3: ((0, 3), (2, 0, 5), (2, 0, 6), (2, 1, 1), (1, 0)),
    4: ((0, 4), (2, 0, 7), (2, 1, 2), (2, 1, 3)),
    5: ((2, 1, 4), (2, 1, 5), (2, 2, 0), (1, 1)),
    6: ((2, 1, 6), (2, 1, 7), (2, 2, 1), (1, 2)),
    7: ((2, 2, 2), (2, 2, 3), (2, 2, 4)),
    8: ((2, 2, 5), (2, 2, 6), (2, 2, 7), (1, 3)),
}


def kernel(
    scale,
    q_hbm, k_hbm, v_hbm, w_hbm, len_ref, o_ref,
    q, kv, wa, wb, start, top, total, accum, attn, mid, give, take, up, down, rup, rdown, tup, tdown,
    load, kv_recv, zp, zm, xs,
    axs, axr, azps, azpr, azms, azmr, bzps, bzpr, bzms, bzmr, bxs, bxr,
    gs, gr, rs, rr,
):
    tok = lax.axis_index("tok")
    head = lax.axis_index("head")
    x, z = lax.div(tok, NZ), lax.rem(tok, NZ)
    y, core = lax.div(head, 2), lax.rem(head, 2)
    rows = q.shape[0]
    ratio = q.shape[1] // HD
    ha = wa.shape[2]

    def at_xz(xx, zz):
        return {"tok": lax.rem(xx + NX, NX) * NZ + lax.rem(zz + NZ, NZ), "head": head}

    def at_y(yy, cc):
        return {"tok": tok, "head": lax.rem(yy + NY, NY) * 2 + cc}

    def remote(src, dst, send, recv, dev):
        return pltpu.make_async_remote_copy(
            src_ref=src, dst_ref=dst, send_sem=send, recv_sem=recv,
            device_id=dev, device_id_type=MESH,
        )

    east, west, south = at_xz(x + 1, z), at_xz(x + 3, z), at_xz(x + 2, z)
    zup, zdown = at_xz(x, z + 1), at_xz(x, z + 7)
    pair = at_y(y, 1 - core)
    yup, ydown = at_y(y + 1, core), at_y(y + 3, core)

    loads = [
        pltpu.make_async_copy(k_hbm, kv.at[0, z, 0], load.at[0]),
        pltpu.make_async_copy(v_hbm, kv.at[0, z, 1], load.at[1]),
        pltpu.make_async_copy(w_hbm.at[pl.ds(0, ha)], wa.at[z, x], load.at[2]),
        pltpu.make_async_copy(w_hbm.at[pl.ds(ha, wb.shape[2])], wb.at[x, z], load.at[3]),
        pltpu.make_async_copy(q_hbm, q, load.at[4]),
    ]
    for c in loads:
        c.start()

    barrier = pltpu.get_barrier_semaphore()
    greeted = (east, west, south, zup, zdown, pair, yup, ydown)
    for dev in greeted:
        pl.semaphore_signal(barrier, inc=1, device_id=dev, device_id_type=MESH)
    pl.semaphore_wait(barrier, len(greeted))

    def kv_zup(zz, p):
        b = kv.at[0, zz, p]
        return remote(b, b, zp.at[zz, p], kv_recv.at[0, zz, p], zup)

    def kv_zdown(zz, p):
        b = kv.at[1, zz, p]
        return remote(b, b, zm.at[zz, p], kv_recv.at[1, zz, p], zdown)

    def kv_east(t, zz, k, p):
        return remote(
            kv.at[t, zz, p], kv.at[t + 1, zz, p], xs.at[k, p], kv_recv.at[t + 1, zz, p], east
        )

    def kv_arrive(t, zz, p):
        b = kv.at[t, zz, p]
        remote(b, b, zp.at[0, p], kv_recv.at[t, zz, p], east).wait_recv()

    def item(k):
        na, nb = z + 1, NZ - z
        m = jnp.minimum(na, nb)
        both = k < 2 * m
        kind = jnp.where(both, lax.rem(k, 2), jnp.where(na > nb, 0, 1))
        j = jnp.where(both, lax.div(k, 2), k - m)
        return kind, jnp.where(kind == 0, z - j, z + j)

    def ax(d):
        return remote(wa.at[z, x], wa.at[z, x], axs.at[d - 1], axr.at[d - 1], at_xz(x + d, z))

    def azp(s):
        b = wa.at[lax.rem(z + NZ - s, NZ)]
        return remote(b, b, azps.at[s], azpr.at[s], zup)

    def azm(s):
        b = wa.at[lax.rem(z + s, NZ)]
        return remote(b, b, azms.at[s], azmr.at[s], zdown)

    def bzp(s):
        b = wb.at[x, lax.rem(z + NZ - s, NZ)]
        return remote(b, b, bzps.at[s], bzpr.at[s], zup)

    def bzm(s):
        b = wb.at[x, lax.rem(z + s, NZ)]
        return remote(b, b, bzms.at[s], bzmr.at[s], zdown)

    order = (0, 1, 7, 2, 6, 3, 5, 4)

    def bx(d, i):
        b = wb.at[lax.rem(x + d, NX), lax.rem(z + order[i], NZ)]
        return remote(b, b, bxs.at[d, i], bxr.at[d, i], west)

    last_up, last_down = lax.rem(z + 1, NZ) < 4, lax.rem(z + 7, NZ) >= 4
    get_up, get_down = z < 4, z >= 4

    def hop(up, down, s):
        if s == 4:

            @pl.when(get_up)
            def _():
                up(3).wait_recv()

            @pl.when(get_down)
            def _():
                down(3).wait_recv()

            return
        if s:
            up(s - 1).wait_recv()
            down(s - 1).wait_recv()
        if s < 3:
            up(s).start()
            down(s).start()
        else:

            @pl.when(last_up)
            def _():
                up(3).start()

            @pl.when(last_down)
            def _():
                down(3).start()

    def relay(kind, s, i=0):
        if kind == 0:
            hop(bzp, bzm, s)
        elif kind == 1:
            if s == 0:
                for d in (1, 2, 3):
                    ax(d).wait_recv()
            hop(azp, azm, s)
        else:
            if s:
                bx(s - 1, i).wait_recv()
            bx(s, i).start()

    for p in (0, 1):
        loads[p].wait()

        @pl.when(z < NZ - 1)
        def _():
            kv_zup(z, p).start()

        @pl.when(x < NX - 1)
        def _():
            kv_east(0, z, 0, p).start()

    loads[3].wait()
    bzp(0).start()
    bzm(0).start()
    bx(0, 0).start()
    loads[2].wait()
    for d in (1, 2, 3):
        ax(d).start()
    loads[4].wait()

    qpos = tok * rows + lax.broadcasted_iota(jnp.int32, (rows, HD), 0)
    edge = jnp.int32(0)
    first = jnp.zeros((rows, HD), jnp.int32)
    for d in range(len_ref.shape[0]):
        edge = edge + len_ref[d]
        first = jnp.maximum(first, jnp.where(qpos >= edge, edge, 0))
    start[...] = first

    lane = lax.broadcasted_iota(jnp.int32, (rows, HD), 1)
    tiles = rows // HD

    def attend(t, zz, fresh):
        base = ((x - t) * NZ + zz) * rows
        kblock = kv[t, zz, 0]
        vblock = kv[t, zz, 1]
        near = start[...] - base
        allowed = []
        for j in range(tiles):
            ok = lane + j * HD >= near
            if fresh:
                ok = ok & (lane + j * HD <= lax.broadcasted_iota(jnp.int32, (rows, HD), 0))
            allowed.append(ok)
        for r in range(ratio):
            s = lax.dot_general(
                q[:, r * HD : (r + 1) * HD], kblock, (((1,), (1,)), ((), ())),
                preferred_element_type=F32,
            )
            parts = [
                jnp.where(allowed[j], s[:, j * HD : (j + 1) * HD], FAR) for j in range(tiles)
            ]
            peak = jnp.max(functools.reduce(jnp.maximum, parts), axis=1, keepdims=True)
            if fresh:
                new = jnp.broadcast_to(peak, (rows, HD))
            else:
                old = top[r]
                new = jnp.maximum(old, peak)
                fade = jnp.exp2((old - new) * scale)
            weights = [jnp.exp2((p - new) * scale) for p in parts]
            added = functools.reduce(jnp.add, weights)
            low = jnp.concatenate([w.astype(BF) for w in weights], axis=1)
            gain = jnp.dot(low, vblock, preferred_element_type=F32)
            top[r] = new
            if fresh:
                total[r] = added
                accum[r] = gain
            else:
                total[r] = total[r] * fade + added
                accum[r] = accum[r] * fade + gain

    attend(0, z, True)

    def step(k, carry):
        have_a = k <= z
        have_b = (x > 0) & (z + k - 1 < NZ)
        az, bz = z - k, z + k - 1

        kind, zz = item(k)
        have_item = (k <= NZ) & (x < NX - 1) & ((kind == 0) | (x > 0))
        for p in (0, 1):

            @pl.when(have_a)
            def _():
                kv_arrive(0, az, p)

            @pl.when(have_a & (z < NZ - 1))
            def _():
                kv_zup(az, p).start()

            @pl.when(have_b)
            def _():
                kv_arrive(1, bz, p)

            @pl.when(have_b & (z > 0))
            def _():
                kv_zdown(bz, p).start()

            @pl.when(have_item)
            def _():
                kv_east(kind, zz, k, p).start()

        for when, moves in PLAN.items():

            @pl.when(k == when)
            def _():
                for move in moves:
                    relay(*move)

        @pl.when(have_a)
        def _():
            attend(0, az, False)

        @pl.when(have_b)
        def _():
            attend(1, bz, False)

        kind, zz = item(k - 1)
        have_x = (k > 1) & (x > 0) & ((kind == 0) | (x > 1))

        @pl.when(have_x)
        def _():
            kv_arrive(kind + 1, zz, 0)
            kv_arrive(kind + 1, zz, 1)
            attend(kind + 1, zz, False)

        return carry

    lax.fori_loop(1, NZ + 2, step, 0)

    for r in range(ratio):
        whole = jnp.sum(total[r], axis=1, keepdims=True)
        attn[:, r * HD : (r + 1) * HD] = (accum[r] / whole).astype(BF)

    for i in range(NZ):
        bx(2, i).wait_recv()
    hop(azp, azm, 4)

    def project(g, c):
        out = []
        for h in (0, 2):
            zz = c * 4 + h
            ra = jnp.concatenate([wa[zz, g], wa[zz + 1, g]], axis=1)
            rb = jnp.concatenate([wb[g, zz], wb[g, zz + 1]], axis=1)
            out.append(
                jnp.dot(attn[:, :ha], ra, preferred_element_type=F32)
                + jnp.dot(attn[:, ha:], rb, preferred_element_type=F32)
            )
        return jnp.concatenate(out, axis=1)

    def swap(i):
        return remote(give.at[i], take.at[i], gs.at[i], gr.at[i], pair)

    half = rows // 2
    lo, hi = pl.ds(0, half), pl.ds(half, half)
    targets = [lax.rem(y + d, NY) for d in (2, 1, 3, 0)]

    def first_pass(i, carry):
        g = lax.rem(y + jnp.where(i == 0, 2, jnp.where(i == 1, 1, jnp.where(i == 2, 3, 0))), NY)
        give[i] = project(g, 1 - core).astype(BF)
        swap(i).start()
        return carry

    lax.fori_loop(0, NY, first_pass, 0)

    far_up = remote(mid.at[lo], rup, rs.at[0], rr.at[0], yup)
    far_down = remote(mid.at[hi], rdown, rs.at[1], rr.at[1], ydown)
    up_hi = remote(up.at[hi], tup.at[hi], rs.at[2], rr.at[2], yup)
    down_lo = remote(down.at[lo], tdown.at[lo], rs.at[3], rr.at[3], ydown)
    up_lo = remote(up.at[lo], tup.at[lo], rs.at[4], rr.at[4], yup)
    down_hi = remote(down.at[hi], tdown.at[hi], rs.at[5], rr.at[5], ydown)

    def both_cores(i):
        mine = project(targets[i], core)
        swap(i).wait_recv()
        return mine + take[i].astype(F32)

    mid[...] = both_cores(0).astype(BF)
    far_up.start()
    far_down.start()
    part = both_cores(1)
    up[hi] = part[half:].astype(BF)
    accum_up = part[:half]
    up_hi.start()
    part = both_cores(2)
    down[lo] = part[:half].astype(BF)
    accum_down = part[half:]
    down_lo.start()
    far_up.wait_recv()
    up[lo] = (accum_up + rup[...].astype(F32)).astype(BF)
    up_lo.start()
    far_down.wait_recv()
    down[hi] = (accum_down + rdown[...].astype(F32)).astype(BF)
    down_hi.start()
    mine = both_cores(3)
    up_hi.wait_recv()
    down_lo.wait_recv()
    up_lo.wait_recv()
    down_hi.wait_recv()
    o_ref[...] = (mine + tup[...].astype(F32) + tdown[...].astype(F32)).astype(BF)

    for i in range(NY):
        swap(i).wait_send()
    for c in (far_up, far_down, up_hi, down_lo, up_lo, down_hi):
        c.wait_send()
    for d in (1, 2, 3):
        ax(d).wait_send()
    for s in range(3):
        for c in (azp(s), azm(s), bzp(s), bzm(s), *(bx(s, i) for i in range(NZ))):
            c.wait_send()

    @pl.when(last_up)
    def _():
        azp(3).wait_send()
        bzp(3).wait_send()

    @pl.when(last_down)
    def _():
        azm(3).wait_send()
        bzm(3).wait_send()

    def drain(k, carry):
        @pl.when((k <= z) & (z < NZ - 1))
        def _():
            kv_zup(k, 0).wait_send()
            kv_zup(k, 1).wait_send()

        @pl.when((k >= z) & (z > 0) & (x > 0) & (k < NZ))
        def _():
            kv_zdown(k, 0).wait_send()
            kv_zdown(k, 1).wait_send()

        kind, zz = item(k)

        @pl.when((x < NX - 1) & ((kind == 0) | (x > 0)))
        def _():
            kv_east(kind, zz, k, 0).wait_send()
            kv_east(kind, zz, k, 1).wait_send()

        return carry

    lax.fori_loop(0, NZ + 1, drain, 0)


def body(queries, keys, values, lengths, out_weight):
    rows, width = queries.shape
    depth = out_weight.shape[0]
    ha = depth * 3 // 8
    scale = math.log2(math.e) / math.sqrt(HD)
    ratio = width // HD
    dma = pltpu.SemaphoreType.DMA
    any_ = pl.BlockSpec(memory_space=pl.ANY)
    return pl.pallas_call(
        functools.partial(kernel, scale),
        out_shape=jax.ShapeDtypeStruct((rows, width), BF),
        in_specs=[any_, any_, any_, any_, pl.BlockSpec(memory_space=pltpu.SMEM)],
        out_specs=pl.BlockSpec(memory_space=pltpu.VMEM),
        scratch_shapes=[
            pltpu.VMEM((rows, width), BF),
            pltpu.VMEM((3, NZ, 2, rows, HD), BF),
            pltpu.VMEM((NZ, NX, ha, HD), BF),
            pltpu.VMEM((NX, NZ, depth - ha, HD), BF),
            pltpu.VMEM((rows, HD), jnp.int32),
            pltpu.VMEM((ratio, rows, HD), F32),
            pltpu.VMEM((ratio, rows, HD), F32),
            pltpu.VMEM((ratio, rows, HD), F32),
            pltpu.VMEM((rows, width), BF),
            pltpu.VMEM((rows, width), BF),
            pltpu.VMEM((NY, rows, width), BF),
            pltpu.VMEM((NY, rows, width), BF),
            pltpu.VMEM((rows, width), BF),
            pltpu.VMEM((rows, width), BF),
            pltpu.VMEM((rows // 2, width), BF),
            pltpu.VMEM((rows // 2, width), BF),
            pltpu.VMEM((rows, width), BF),
            pltpu.VMEM((rows, width), BF),
            dma((5,)), dma((3, NZ, 2)), dma((NZ, 2)), dma((NZ, 2)), dma((NZ + 1, 2)),
            dma((3,)), dma((3,)),
            dma((4,)), dma((4,)), dma((4,)), dma((4,)),
            dma((4,)), dma((4,)), dma((4,)), dma((4,)),
            dma((3, NZ)), dma((3, NZ)),
            dma((NY,)), dma((NY,)), dma((6,)), dma((6,)),
        ],
        compiler_params=pltpu.CompilerParams(
            collective_id=0, has_side_effects=True, vmem_limit_bytes=60 * 1024 * 1024
        ),
    )(queries, keys, values, out_weight, lengths)


def solution(mesh):
    placed = (P("tok", "head"), P("tok", "head"), P("tok", "head"), P(), P("head", "tok"))
    return jax.shard_map(
        body, mesh=mesh, in_specs=placed, out_specs=P("tok", "head"), check_vma=False
    )
```

```python
import functools
import math

import jax
import jax.numpy as jnp
from jax import lax
from jax.experimental import pallas as pl
from jax.experimental.pallas import tpu as pltpu
from jax.sharding import PartitionSpec as P

HD = 128
NX, NZ, NY = 4, 8, 4
MESH = pl.DeviceIdType.MESH
FAR = -1e30
BF = jnp.bfloat16
F32 = jnp.float32
PLAN = {
    1: ((0, 1), (2, 0, 1), (2, 0, 2)),
    2: ((0, 2), (2, 0, 3), (2, 0, 4), (2, 1, 0)),
    3: ((0, 3), (2, 0, 5), (2, 0, 6), (2, 1, 1), (1, 0)),
    4: ((0, 4), (2, 0, 7), (2, 1, 2), (2, 1, 3)),
    5: ((2, 1, 4), (2, 1, 5), (2, 2, 0), (1, 1)),
    6: ((2, 1, 6), (2, 1, 7), (2, 2, 1), (1, 2)),
    7: ((2, 2, 2), (2, 2, 3), (2, 2, 4)),
    8: ((2, 2, 5), (2, 2, 6), (2, 2, 7), (1, 3)),
}


def kernel(
    scale,
    q_hbm, k_hbm, v_hbm, w_hbm, len_ref, o_ref,
    q, kv, wa, wb, start, top, total, accum, attn, mid, give, take, up, down, rup, rdown, tup, tdown,
    load, kv_recv, zp, zm, xs,
    axs, axr, azps, azpr, azms, azmr, bzps, bzpr, bzms, bzmr, bxs, bxr,
    gs, gr, rs, rr,
):
    tok = lax.axis_index("tok")
    head = lax.axis_index("head")
    x, z = lax.div(tok, NZ), lax.rem(tok, NZ)
    y, core = lax.div(head, 2), lax.rem(head, 2)
    rows = q.shape[0]
    ratio = q.shape[1] // HD
    ha = wa.shape[2]

    def at_xz(xx, zz):
        return {"tok": lax.rem(xx + NX, NX) * NZ + lax.rem(zz + NZ, NZ), "head": head}

    def at_y(yy, cc):
        return {"tok": tok, "head": lax.rem(yy + NY, NY) * 2 + cc}

    def remote(src, dst, send, recv, dev):
        return pltpu.make_async_remote_copy(
            src_ref=src, dst_ref=dst, send_sem=send, recv_sem=recv,
            device_id=dev, device_id_type=MESH,
        )

    east, west, south = at_xz(x + 1, z), at_xz(x + 3, z), at_xz(x + 2, z)
    zup, zdown = at_xz(x, z + 1), at_xz(x, z + 7)
    pair = at_y(y, 1 - core)
    yup, ydown = at_y(y + 1, core), at_y(y + 3, core)

    loads = [
        pltpu.make_async_copy(k_hbm, kv.at[0, z, 0], load.at[0]),
        pltpu.make_async_copy(v_hbm, kv.at[0, z, 1], load.at[1]),
        pltpu.make_async_copy(w_hbm.at[pl.ds(0, ha)], wa.at[z, x], load.at[2]),
        pltpu.make_async_copy(w_hbm.at[pl.ds(ha, wb.shape[2])], wb.at[x, z], load.at[3]),
        pltpu.make_async_copy(q_hbm, q, load.at[4]),
    ]
    for c in loads:
        c.start()

    barrier = pltpu.get_barrier_semaphore()
    greeted = (east, west, south, zup, zdown, pair, yup, ydown)
    for dev in greeted:
        pl.semaphore_signal(barrier, inc=1, device_id=dev, device_id_type=MESH)
    pl.semaphore_wait(barrier, len(greeted))

    def kv_zup(zz, p):
        b = kv.at[0, zz, p]
        return remote(b, b, zp.at[zz, p], kv_recv.at[0, zz, p], zup)

    def kv_zdown(zz, p):
        b = kv.at[1, zz, p]
        return remote(b, b, zm.at[zz, p], kv_recv.at[1, zz, p], zdown)

    def kv_east(t, zz, k, p):
        return remote(
            kv.at[t, zz, p], kv.at[t + 1, zz, p], xs.at[k, p], kv_recv.at[t + 1, zz, p], east
        )

    def kv_arrive(t, zz, p):
        b = kv.at[t, zz, p]
        remote(b, b, zp.at[0, p], kv_recv.at[t, zz, p], east).wait_recv()

    def item(k):
        na, nb = z + 1, NZ - z
        m = jnp.minimum(na, nb)
        both = k < 2 * m
        kind = jnp.where(both, lax.rem(k, 2), jnp.where(na > nb, 0, 1))
        j = jnp.where(both, lax.div(k, 2), k - m)
        return kind, jnp.where(kind == 0, z - j, z + j)

    def kv_first(p):
        b = kv.at[0, 0, p]
        return remote(b, b, zm.at[0, p], kv_recv.at[0, 0, p], zdown)

    def kv_last(p):
        b = kv.at[1, NZ - 1, p]
        return remote(b, b, zp.at[NZ - 1, p], kv_recv.at[1, NZ - 1, p], zup)

    def ax(d):
        return remote(wa.at[z, x], wa.at[z, x], axs.at[d - 1], axr.at[d - 1], at_xz(x + d, z))

    def azp(s):
        b = wa.at[lax.rem(z + NZ - s, NZ)]
        return remote(b, b, azps.at[s], azpr.at[s], zup)

    def azm(s):
        b = wa.at[lax.rem(z + s, NZ)]
        return remote(b, b, azms.at[s], azmr.at[s], zdown)

    def bzp(s):
        b = wb.at[x, lax.rem(z + NZ - s, NZ)]
        return remote(b, b, bzps.at[s], bzpr.at[s], zup)

    def bzm(s):
        b = wb.at[x, lax.rem(z + s, NZ)]
        return remote(b, b, bzms.at[s], bzmr.at[s], zdown)

    order = (0, 1, 7, 2, 6, 3, 5, 4)

    def bx(d, i):
        b = wb.at[lax.rem(x + d, NX), lax.rem(z + order[i], NZ)]
        return remote(b, b, bxs.at[d, i], bxr.at[d, i], west)

    last_up, last_down = lax.rem(z + 1, NZ) < 4, lax.rem(z + 7, NZ) >= 4
    get_up, get_down = z < 4, z >= 4

    def hop(up, down, s):
        if s == 4:

            @pl.when(get_up)
            def _():
                up(3).wait_recv()

            @pl.when(get_down)
            def _():
                down(3).wait_recv()

            return
        if s:
            up(s - 1).wait_recv()
            down(s - 1).wait_recv()
        if s < 3:
            up(s).start()
            down(s).start()
        else:

            @pl.when(last_up)
            def _():
                up(3).start()

            @pl.when(last_down)
            def _():
                down(3).start()

    def relay(kind, s, i=0):
        if kind == 0:
            hop(bzp, bzm, s)
        elif kind == 1:
            if s == 0:
                for d in (1, 2, 3):
                    ax(d).wait_recv()
            hop(azp, azm, s)
        else:
            if s:
                bx(s - 1, i).wait_recv()
            bx(s, i).start()

    for p in (0, 1):
        loads[p].wait()

        @pl.when(z < NZ - 1)
        def _():
            kv_zup(z, p).start()

        @pl.when(z == 0)
        def _():
            kv_first(p).start()

        @pl.when(x < NX - 1)
        def _():
            kv_east(0, z, 0, p).start()

    loads[3].wait()
    bzp(0).start()
    bzm(0).start()
    bx(0, 0).start()
    loads[2].wait()
    for d in (1, 2, 3):
        ax(d).start()
    loads[4].wait()

    qpos = tok * rows + lax.broadcasted_iota(jnp.int32, (rows, HD), 0)
    edge = jnp.int32(0)
    first = jnp.zeros((rows, HD), jnp.int32)
    for d in range(len_ref.shape[0]):
        edge = edge + len_ref[d]
        first = jnp.maximum(first, jnp.where(qpos >= edge, edge, 0))
    start[...] = first

    lane = lax.broadcasted_iota(jnp.int32, (rows, HD), 1)
    tiles = rows // HD

    def attend(t, zz, fresh):
        base = ((x - t) * NZ + zz) * rows
        kblock = kv[t, zz, 0]
        vblock = kv[t, zz, 1]
        near = start[...] - base
        allowed = []
        for j in range(tiles):
            ok = lane + j * HD >= near
            if fresh:
                ok = ok & (lane + j * HD <= lax.broadcasted_iota(jnp.int32, (rows, HD), 0))
            allowed.append(ok)
        for r in range(ratio):
            s = lax.dot_general(
                q[:, r * HD : (r + 1) * HD], kblock, (((1,), (1,)), ((), ())),
                preferred_element_type=F32,
            )
            parts = [
                jnp.where(allowed[j], s[:, j * HD : (j + 1) * HD], FAR) for j in range(tiles)
            ]
            peak = jnp.max(functools.reduce(jnp.maximum, parts), axis=1, keepdims=True)
            if fresh:
                new = jnp.broadcast_to(peak, (rows, HD))
            else:
                old = top[r]
                new = jnp.maximum(old, peak)
                fade = jnp.exp2((old - new) * scale)
            weights = [jnp.exp2((p - new) * scale) for p in parts]
            added = functools.reduce(jnp.add, weights)
            low = jnp.concatenate([w.astype(BF) for w in weights], axis=1)
            gain = jnp.dot(low, vblock, preferred_element_type=F32)
            top[r] = new
            if fresh:
                total[r] = added
                accum[r] = gain
            else:
                total[r] = total[r] * fade + added
                accum[r] = accum[r] * fade + gain

    attend(0, z, True)

    def step(k, carry):
        have_a = k <= z
        have_b = (x > 0) & (z + k - 1 < NZ) & ((z > 0) | (k < NZ))
        have_r = (x > 0) & (z == 0) & (k == 2)
        az, bz = z - k, z + k - 1

        kind, zz = item(k)
        have_item = (k <= NZ) & (x < NX - 1) & ((kind == 0) | (x > 0))
        for p in (0, 1):

            @pl.when(have_a)
            def _():
                kv_arrive(0, az, p)

            @pl.when(have_a & (z < NZ - 1) & ((z < NZ - 2) | (az > 0)))
            def _():
                kv_zup(az, p).start()

            @pl.when(have_b)
            def _():
                kv_arrive(1, bz, p)

            @pl.when(have_b & (z > 0) & ((z > 1) | (bz < NZ - 1)))
            def _():
                kv_zdown(bz, p).start()

            @pl.when((k == 1) & (x > 0) & (z == NZ - 1))
            def _():
                kv_last(p).start()

            @pl.when(have_r)
            def _():
                kv_arrive(1, NZ - 1, p)

            @pl.when(have_item)
            def _():
                kv_east(kind, zz, k, p).start()

        for when, moves in PLAN.items():

            @pl.when(k == when)
            def _():
                for move in moves:
                    relay(*move)

        @pl.when(have_a)
        def _():
            attend(0, az, False)

        @pl.when(have_b)
        def _():
            attend(1, bz, False)

        @pl.when(have_r)
        def _():
            attend(1, NZ - 1, False)

        kind, zz = item(k - 1)
        have_x = (k > 1) & (x > 0) & ((kind == 0) | (x > 1))

        @pl.when(have_x)
        def _():
            kv_arrive(kind + 1, zz, 0)
            kv_arrive(kind + 1, zz, 1)
            attend(kind + 1, zz, False)

        return carry

    lax.fori_loop(1, NZ + 2, step, 0)

    for r in range(ratio):
        whole = jnp.sum(total[r], axis=1, keepdims=True)
        attn[:, r * HD : (r + 1) * HD] = (accum[r] / whole).astype(BF)

    for i in range(NZ):
        bx(2, i).wait_recv()
    hop(azp, azm, 4)

    def project(g, c):
        out = []
        for h in (0, 2):
            zz = c * 4 + h
            ra = jnp.concatenate([wa[zz, g], wa[zz + 1, g]], axis=1)
            rb = jnp.concatenate([wb[g, zz], wb[g, zz + 1]], axis=1)
            out.append(
                jnp.dot(attn[:, :ha], ra, preferred_element_type=F32)
                + jnp.dot(attn[:, ha:], rb, preferred_element_type=F32)
            )
        return jnp.concatenate(out, axis=1)

    def swap(i):
        return remote(give.at[i], take.at[i], gs.at[i], gr.at[i], pair)

    half = rows // 2
    lo, hi = pl.ds(0, half), pl.ds(half, half)
    targets = [lax.rem(y + d, NY) for d in (2, 1, 3, 0)]

    def first_pass(i, carry):
        g = lax.rem(y + jnp.where(i == 0, 2, jnp.where(i == 1, 1, jnp.where(i == 2, 3, 0))), NY)
        give[i] = project(g, 1 - core).astype(BF)
        swap(i).start()
        return carry

    lax.fori_loop(0, NY, first_pass, 0)

    far_up = remote(mid.at[lo], rup, rs.at[0], rr.at[0], yup)
    far_down = remote(mid.at[hi], rdown, rs.at[1], rr.at[1], ydown)
    up_hi = remote(up.at[hi], tup.at[hi], rs.at[2], rr.at[2], yup)
    down_lo = remote(down.at[lo], tdown.at[lo], rs.at[3], rr.at[3], ydown)
    up_lo = remote(up.at[lo], tup.at[lo], rs.at[4], rr.at[4], yup)
    down_hi = remote(down.at[hi], tdown.at[hi], rs.at[5], rr.at[5], ydown)

    def both_cores(i):
        mine = project(targets[i], core)
        swap(i).wait_recv()
        return mine + take[i].astype(F32)

    mid[...] = both_cores(0).astype(BF)
    far_up.start()
    far_down.start()
    part = both_cores(1)
    up[hi] = part[half:].astype(BF)
    accum_up = part[:half]
    up_hi.start()
    part = both_cores(2)
    down[lo] = part[:half].astype(BF)
    accum_down = part[half:]
    down_lo.start()
    far_up.wait_recv()
    up[lo] = (accum_up + rup[...].astype(F32)).astype(BF)
    up_lo.start()
    far_down.wait_recv()
    down[hi] = (accum_down + rdown[...].astype(F32)).astype(BF)
    down_hi.start()
    mine = both_cores(3)
    up_hi.wait_recv()
    down_lo.wait_recv()
    up_lo.wait_recv()
    down_hi.wait_recv()
    o_ref[...] = (mine + tup[...].astype(F32) + tdown[...].astype(F32)).astype(BF)

    for i in range(NY):
        swap(i).wait_send()
    for c in (far_up, far_down, up_hi, down_lo, up_lo, down_hi):
        c.wait_send()
    for d in (1, 2, 3):
        ax(d).wait_send()
    for s in range(3):
        for c in (azp(s), azm(s), bzp(s), bzm(s), *(bx(s, i) for i in range(NZ))):
            c.wait_send()

    @pl.when(last_up)
    def _():
        azp(3).wait_send()
        bzp(3).wait_send()

    @pl.when(last_down)
    def _():
        azm(3).wait_send()
        bzm(3).wait_send()

    def drain(k, carry):
        @pl.when((k <= z) & (z < NZ - 1) & ((z < NZ - 2) | (k > 0)))
        def _():
            for p in (0, 1):
                kv_zup(k, p).wait_send()

        @pl.when((k >= z) & (z > 0) & (x > 0) & (k < NZ) & ((z > 1) | (k < NZ - 1)))
        def _():
            for p in (0, 1):
                kv_zdown(k, p).wait_send()

        @pl.when((k == 0) & (z == 0))
        def _():
            for p in (0, 1):
                kv_first(p).wait_send()

        @pl.when((k == 0) & (x > 0) & (z == NZ - 1))
        def _():
            for p in (0, 1):
                kv_last(p).wait_send()

        kind, zz = item(k)

        @pl.when((x < NX - 1) & ((kind == 0) | (x > 0)))
        def _():
            kv_east(kind, zz, k, 0).wait_send()
            kv_east(kind, zz, k, 1).wait_send()

        return carry

    lax.fori_loop(0, NZ + 1, drain, 0)


def body(queries, keys, values, lengths, out_weight):
    rows, width = queries.shape
    depth = out_weight.shape[0]
    ha = depth * 3 // 8
    scale = math.log2(math.e) / math.sqrt(HD)
    ratio = width // HD
    dma = pltpu.SemaphoreType.DMA
    any_ = pl.BlockSpec(memory_space=pl.ANY)
    return pl.pallas_call(
        functools.partial(kernel, scale),
        out_shape=jax.ShapeDtypeStruct((rows, width), BF),
        in_specs=[any_, any_, any_, any_, pl.BlockSpec(memory_space=pltpu.SMEM)],
        out_specs=pl.BlockSpec(memory_space=pltpu.VMEM),
        scratch_shapes=[
            pltpu.VMEM((rows, width), BF),
            pltpu.VMEM((3, NZ, 2, rows, HD), BF),
            pltpu.VMEM((NZ, NX, ha, HD), BF),
            pltpu.VMEM((NX, NZ, depth - ha, HD), BF),
            pltpu.VMEM((rows, HD), jnp.int32),
            pltpu.VMEM((ratio, rows, HD), F32),
            pltpu.VMEM((ratio, rows, HD), F32),
            pltpu.VMEM((ratio, rows, HD), F32),
            pltpu.VMEM((rows, width), BF),
            pltpu.VMEM((rows, width), BF),
            pltpu.VMEM((NY, rows, width), BF),
            pltpu.VMEM((NY, rows, width), BF),
            pltpu.VMEM((rows, width), BF),
            pltpu.VMEM((rows, width), BF),
            pltpu.VMEM((rows // 2, width), BF),
            pltpu.VMEM((rows // 2, width), BF),
            pltpu.VMEM((rows, width), BF),
            pltpu.VMEM((rows, width), BF),
            dma((5,)), dma((3, NZ, 2)), dma((NZ, 2)), dma((NZ, 2)), dma((NZ + 1, 2)),
            dma((3,)), dma((3,)),
            dma((4,)), dma((4,)), dma((4,)), dma((4,)),
            dma((4,)), dma((4,)), dma((4,)), dma((4,)),
            dma((3, NZ)), dma((3, NZ)),
            dma((NY,)), dma((NY,)), dma((6,)), dma((6,)),
        ],
        compiler_params=pltpu.CompilerParams(
            collective_id=0, has_side_effects=True, vmem_limit_bytes=60 * 1024 * 1024
        ),
    )(queries, keys, values, out_weight, lengths)


def solution(mesh):
    placed = (P("tok", "head"), P("tok", "head"), P("tok", "head"), P(), P("head", "tok"))
    return jax.shard_map(
        body, mesh=mesh, in_specs=placed, out_specs=P("tok", "head"), check_vma=False
    )
```

```python
import functools
import math

import jax
import jax.numpy as jnp
from jax import lax
from jax.experimental import pallas as pl
from jax.experimental.pallas import tpu as pltpu
from jax.sharding import PartitionSpec as P

HD = 128
NX, NZ, NY = 4, 8, 4
MESH = pl.DeviceIdType.MESH
FAR = -1e30
BF = jnp.bfloat16
F32 = jnp.float32
PLAN = {
    1: ((0, 1), (2, 0, 1), (2, 0, 2), (2, 1, 0)),
    2: ((0, 2), (2, 0, 3), (2, 0, 4), (2, 1, 1), (2, 1, 2), (1, 0)),
    3: ((0, 3), (2, 0, 5), (2, 1, 3), (2, 1, 4), (2, 2, 1)),
    4: ((0, 4), (2, 0, 6), (2, 1, 5), (1, 1)),
    5: ((2, 0, 7), (2, 1, 6), (2, 2, 2), (2, 2, 4), (2, 2, 5)),
    6: ((1, 2),),
    7: ((2, 1, 7), (2, 2, 0)),
    8: ((2, 2, 3), (2, 2, 6), (2, 2, 7), (1, 3)),
}


def kernel(
    scale,
    q_hbm, k_hbm, v_hbm, w_hbm, len_ref, o_ref,
    q, kv, wa, wb, start, top, total, accum, attn, mid, give, take, up, down, rup, rdown, tup, tdown,
    load, kv_recv, zp, zm, xs,
    axs, axr, azps, azpr, azms, azmr, bzps, bzpr, bzms, bzmr, bxs, bxr,
    gs, gr, rs, rr,
):
    tok = lax.axis_index("tok")
    head = lax.axis_index("head")
    x, z = lax.div(tok, NZ), lax.rem(tok, NZ)
    y, core = lax.div(head, 2), lax.rem(head, 2)
    rows = q.shape[0]
    ratio = q.shape[1] // HD
    ha = wa.shape[2]

    def at_xz(xx, zz):
        return {"tok": lax.rem(xx + NX, NX) * NZ + lax.rem(zz + NZ, NZ), "head": head}

    def at_y(yy, cc):
        return {"tok": tok, "head": lax.rem(yy + NY, NY) * 2 + cc}

    def remote(src, dst, send, recv, dev):
        return pltpu.make_async_remote_copy(
            src_ref=src, dst_ref=dst, send_sem=send, recv_sem=recv,
            device_id=dev, device_id_type=MESH,
        )

    east, west, south = at_xz(x + 1, z), at_xz(x + 3, z), at_xz(x + 2, z)
    zup, zdown = at_xz(x, z + 1), at_xz(x, z + 7)
    pair = at_y(y, 1 - core)
    yup, ydown = at_y(y + 1, core), at_y(y + 3, core)

    loads = [
        pltpu.make_async_copy(k_hbm, kv.at[0, z, 0], load.at[0]),
        pltpu.make_async_copy(v_hbm, kv.at[0, z, 1], load.at[1]),
        pltpu.make_async_copy(w_hbm.at[pl.ds(0, ha)], wa.at[z, x], load.at[2]),
        pltpu.make_async_copy(w_hbm.at[pl.ds(ha, wb.shape[2])], wb.at[x, z], load.at[3]),
        pltpu.make_async_copy(q_hbm, q, load.at[4]),
    ]
    for c in loads:
        c.start()

    barrier = pltpu.get_barrier_semaphore()
    greeted = (east, west, south, zup, zdown, pair, yup, ydown)
    for dev in greeted:
        pl.semaphore_signal(barrier, inc=1, device_id=dev, device_id_type=MESH)
    pl.semaphore_wait(barrier, len(greeted))

    def kv_zup(zz, p):
        b = kv.at[0, zz, p]
        return remote(b, b, zp.at[zz, p], kv_recv.at[0, zz, p], zup)

    def kv_zdown(zz, p):
        b = kv.at[1, zz, p]
        return remote(b, b, zm.at[zz, p], kv_recv.at[1, zz, p], zdown)

    def kv_east(t, zz, k, p):
        return remote(
            kv.at[t, zz, p], kv.at[t + 1, zz, p], xs.at[k, p], kv_recv.at[t + 1, zz, p], east
        )

    def kv_arrive(t, zz, p):
        b = kv.at[t, zz, p]
        remote(b, b, zp.at[0, p], kv_recv.at[t, zz, p], east).wait_recv()

    def item(k):
        na, nb = z + 1, NZ - z
        m = jnp.minimum(na, nb)
        both = k < 2 * m
        kind = jnp.where(both, lax.rem(k, 2), jnp.where(na > nb, 0, 1))
        j = jnp.where(both, lax.div(k, 2), k - m)
        return kind, jnp.where(kind == 0, z - j, z + j)

    def kv_first(p):
        b = kv.at[0, 0, p]
        return remote(b, b, zm.at[0, p], kv_recv.at[0, 0, p], zdown)

    def kv_last(p):
        b = kv.at[1, NZ - 1, p]
        return remote(b, b, zp.at[NZ - 1, p], kv_recv.at[1, NZ - 1, p], zup)

    def ax(d):
        return remote(wa.at[z, x], wa.at[z, x], axs.at[d - 1], axr.at[d - 1], at_xz(x + d, z))

    def azp(s):
        b = wa.at[lax.rem(z + NZ - s, NZ)]
        return remote(b, b, azps.at[s], azpr.at[s], zup)

    def azm(s):
        b = wa.at[lax.rem(z + s, NZ)]
        return remote(b, b, azms.at[s], azmr.at[s], zdown)

    def bzp(s):
        b = wb.at[x, lax.rem(z + NZ - s, NZ)]
        return remote(b, b, bzps.at[s], bzpr.at[s], zup)

    def bzm(s):
        b = wb.at[x, lax.rem(z + s, NZ)]
        return remote(b, b, bzms.at[s], bzmr.at[s], zdown)

    order = (0, 1, 7, 2, 6, 3, 5, 4)

    def bx(d, i):
        b = wb.at[lax.rem(x + d, NX), lax.rem(z + order[i], NZ)]
        return remote(b, b, bxs.at[d, i], bxr.at[d, i], west)

    last_up, last_down = lax.rem(z + 1, NZ) < 4, lax.rem(z + 7, NZ) >= 4
    get_up, get_down = z < 4, z >= 4

    def hop(up, down, s):
        if s == 4:

            @pl.when(get_up)
            def _():
                up(3).wait_recv()

            @pl.when(get_down)
            def _():
                down(3).wait_recv()

            return
        if s:
            up(s - 1).wait_recv()
            down(s - 1).wait_recv()
        if s < 3:
            up(s).start()
            down(s).start()
        else:

            @pl.when(last_up)
            def _():
                up(3).start()

            @pl.when(last_down)
            def _():
                down(3).start()

    def relay(kind, s, i=0):
        if kind == 0:
            hop(bzp, bzm, s)
        elif kind == 1:
            if s == 0:
                for d in (1, 2, 3):
                    ax(d).wait_recv()
            hop(azp, azm, s)
        else:
            if s:
                bx(s - 1, i).wait_recv()
            bx(s, i).start()

    for p in (0, 1):
        loads[p].wait()

        @pl.when(z < NZ - 1)
        def _():
            kv_zup(z, p).start()

        @pl.when(z == 0)
        def _():
            kv_first(p).start()

        @pl.when(x < NX - 1)
        def _():
            kv_east(0, z, 0, p).start()

    loads[3].wait()
    bzp(0).start()
    bzm(0).start()
    bx(0, 0).start()
    loads[2].wait()
    for d in (1, 2, 3):
        ax(d).start()
    loads[4].wait()

    qpos = tok * rows + lax.broadcasted_iota(jnp.int32, (rows, HD), 0)
    edge = jnp.int32(0)
    first = jnp.zeros((rows, HD), jnp.int32)
    for d in range(len_ref.shape[0]):
        edge = edge + len_ref[d]
        first = jnp.maximum(first, jnp.where(qpos >= edge, edge, 0))
    start[...] = first

    lane = lax.broadcasted_iota(jnp.int32, (rows, HD), 1)
    tiles = rows // HD

    def attend(t, zz, fresh):
        base = ((x - t) * NZ + zz) * rows
        kblock = kv[t, zz, 0]
        vblock = kv[t, zz, 1]
        near = start[...] - base
        allowed = []
        for j in range(tiles):
            ok = lane + j * HD >= near
            if fresh:
                ok = ok & (lane + j * HD <= lax.broadcasted_iota(jnp.int32, (rows, HD), 0))
            allowed.append(ok)
        for r in range(ratio):
            s = lax.dot_general(
                q[:, r * HD : (r + 1) * HD], kblock, (((1,), (1,)), ((), ())),
                preferred_element_type=F32,
            )
            parts = [
                jnp.where(allowed[j], s[:, j * HD : (j + 1) * HD], FAR) for j in range(tiles)
            ]
            peak = jnp.max(functools.reduce(jnp.maximum, parts), axis=1, keepdims=True)
            if fresh:
                new = jnp.broadcast_to(peak, (rows, HD))
            else:
                old = top[r]
                new = jnp.maximum(old, peak)
                fade = jnp.exp2((old - new) * scale)
            weights = [jnp.exp2((p - new) * scale) for p in parts]
            added = functools.reduce(jnp.add, weights)
            low = jnp.concatenate([w.astype(BF) for w in weights], axis=1)
            gain = jnp.dot(low, vblock, preferred_element_type=F32)
            top[r] = new
            if fresh:
                total[r] = added
                accum[r] = gain
            else:
                total[r] = total[r] * fade + added
                accum[r] = accum[r] * fade + gain

    attend(0, z, True)

    def step(k, carry):
        have_a = k <= z
        have_b = (x > 0) & (z + k - 1 < NZ) & ((z > 0) | (k < NZ))
        have_r = (x > 0) & (z == 0) & (k == 2)
        az, bz = z - k, z + k - 1

        kind, zz = item(k)
        have_item = (k <= NZ) & (x < NX - 1) & ((kind == 0) | (x > 0))
        for p in (0, 1):

            @pl.when(have_a)
            def _():
                kv_arrive(0, az, p)

            @pl.when(have_a & (z < NZ - 1) & ((z < NZ - 2) | (az > 0)))
            def _():
                kv_zup(az, p).start()

            @pl.when(have_b)
            def _():
                kv_arrive(1, bz, p)

            @pl.when(have_b & (z > 0) & ((z > 1) | (bz < NZ - 1)))
            def _():
                kv_zdown(bz, p).start()

            @pl.when((k == 1) & (x > 0) & (z == NZ - 1))
            def _():
                kv_last(p).start()

            @pl.when(have_r)
            def _():
                kv_arrive(1, NZ - 1, p)

            @pl.when(have_item)
            def _():
                kv_east(kind, zz, k, p).start()

        for when, moves in PLAN.items():

            @pl.when(k == when)
            def _():
                for move in moves:
                    relay(*move)

        @pl.when(have_a)
        def _():
            attend(0, az, False)

        @pl.when(have_b)
        def _():
            attend(1, bz, False)

        @pl.when(have_r)
        def _():
            attend(1, NZ - 1, False)

        kind, zz = item(k - 1)
        have_x = (k > 1) & (x > 0) & ((kind == 0) | (x > 1))

        @pl.when(have_x)
        def _():
            kv_arrive(kind + 1, zz, 0)
            kv_arrive(kind + 1, zz, 1)
            attend(kind + 1, zz, False)

        return carry

    lax.fori_loop(1, NZ + 2, step, 0)

    for r in range(ratio):
        whole = jnp.sum(total[r], axis=1, keepdims=True)
        attn[:, r * HD : (r + 1) * HD] = (accum[r] / whole).astype(BF)

    for i in range(NZ):
        bx(2, i).wait_recv()
    hop(azp, azm, 4)

    def project(g, c):
        out = []
        for h in (0, 2):
            zz = c * 4 + h
            ra = jnp.concatenate([wa[zz, g], wa[zz + 1, g]], axis=1)
            rb = jnp.concatenate([wb[g, zz], wb[g, zz + 1]], axis=1)
            out.append(
                jnp.dot(attn[:, :ha], ra, preferred_element_type=F32)
                + jnp.dot(attn[:, ha:], rb, preferred_element_type=F32)
            )
        return jnp.concatenate(out, axis=1)

    def swap(i):
        return remote(give.at[i], take.at[i], gs.at[i], gr.at[i], pair)

    half = rows // 2
    lo, hi = pl.ds(0, half), pl.ds(half, half)
    targets = [lax.rem(y + d, NY) for d in (2, 1, 3, 0)]

    def first_pass(i, carry):
        g = lax.rem(y + jnp.where(i == 0, 2, jnp.where(i == 1, 1, jnp.where(i == 2, 3, 0))), NY)
        give[i] = project(g, 1 - core).astype(BF)
        swap(i).start()
        return carry

    lax.fori_loop(0, NY, first_pass, 0)

    far_up = remote(mid.at[lo], rup, rs.at[0], rr.at[0], yup)
    far_down = remote(mid.at[hi], rdown, rs.at[1], rr.at[1], ydown)
    up_hi = remote(up.at[hi], tup.at[hi], rs.at[2], rr.at[2], yup)
    down_lo = remote(down.at[lo], tdown.at[lo], rs.at[3], rr.at[3], ydown)
    up_lo = remote(up.at[lo], tup.at[lo], rs.at[4], rr.at[4], yup)
    down_hi = remote(down.at[hi], tdown.at[hi], rs.at[5], rr.at[5], ydown)

    def both_cores(i):
        mine = project(targets[i], core)
        swap(i).wait_recv()
        return mine + take[i].astype(F32)

    mid[...] = both_cores(0).astype(BF)
    far_up.start()
    far_down.start()
    part = both_cores(1)
    up[hi] = part[half:].astype(BF)
    accum_up = part[:half]
    up_hi.start()
    part = both_cores(2)
    down[lo] = part[:half].astype(BF)
    accum_down = part[half:]
    down_lo.start()
    far_up.wait_recv()
    up[lo] = (accum_up + rup[...].astype(F32)).astype(BF)
    up_lo.start()
    far_down.wait_recv()
    down[hi] = (accum_down + rdown[...].astype(F32)).astype(BF)
    down_hi.start()
    mine = both_cores(3)
    up_hi.wait_recv()
    down_lo.wait_recv()
    up_lo.wait_recv()
    down_hi.wait_recv()
    o_ref[...] = (mine + tup[...].astype(F32) + tdown[...].astype(F32)).astype(BF)

    for i in range(NY):
        swap(i).wait_send()
    for c in (far_up, far_down, up_hi, down_lo, up_lo, down_hi):
        c.wait_send()
    for d in (1, 2, 3):
        ax(d).wait_send()
    for s in range(3):
        for c in (azp(s), azm(s), bzp(s), bzm(s), *(bx(s, i) for i in range(NZ))):
            c.wait_send()

    @pl.when(last_up)
    def _():
        azp(3).wait_send()
        bzp(3).wait_send()

    @pl.when(last_down)
    def _():
        azm(3).wait_send()
        bzm(3).wait_send()

    def drain(k, carry):
        @pl.when((k <= z) & (z < NZ - 1) & ((z < NZ - 2) | (k > 0)))
        def _():
            for p in (0, 1):
                kv_zup(k, p).wait_send()

        @pl.when((k >= z) & (z > 0) & (x > 0) & (k < NZ) & ((z > 1) | (k < NZ - 1)))
        def _():
            for p in (0, 1):
                kv_zdown(k, p).wait_send()

        @pl.when((k == 0) & (z == 0))
        def _():
            for p in (0, 1):
                kv_first(p).wait_send()

        @pl.when((k == 0) & (x > 0) & (z == NZ - 1))
        def _():
            for p in (0, 1):
                kv_last(p).wait_send()

        kind, zz = item(k)

        @pl.when((x < NX - 1) & ((kind == 0) | (x > 0)))
        def _():
            kv_east(kind, zz, k, 0).wait_send()
            kv_east(kind, zz, k, 1).wait_send()

        return carry

    lax.fori_loop(0, NZ + 1, drain, 0)


def body(queries, keys, values, lengths, out_weight):
    rows, width = queries.shape
    depth = out_weight.shape[0]
    ha = depth * 11 // 32
    scale = math.log2(math.e) / math.sqrt(HD)
    ratio = width // HD
    dma = pltpu.SemaphoreType.DMA
    any_ = pl.BlockSpec(memory_space=pl.ANY)
    return pl.pallas_call(
        functools.partial(kernel, scale),
        out_shape=jax.ShapeDtypeStruct((rows, width), BF),
        in_specs=[any_, any_, any_, any_, pl.BlockSpec(memory_space=pltpu.SMEM)],
        out_specs=pl.BlockSpec(memory_space=pltpu.VMEM),
        scratch_shapes=[
            pltpu.VMEM((rows, width), BF),
            pltpu.VMEM((3, NZ, 2, rows, HD), BF),
            pltpu.VMEM((NZ, NX, ha, HD), BF),
            pltpu.VMEM((NX, NZ, depth - ha, HD), BF),
            pltpu.VMEM((rows, HD), jnp.int32),
            pltpu.VMEM((ratio, rows, HD), F32),
            pltpu.VMEM((ratio, rows, HD), F32),
            pltpu.VMEM((ratio, rows, HD), F32),
            pltpu.VMEM((rows, width), BF),
            pltpu.VMEM((rows, width), BF),
            pltpu.VMEM((NY, rows, width), BF),
            pltpu.VMEM((NY, rows, width), BF),
            pltpu.VMEM((rows, width), BF),
            pltpu.VMEM((rows, width), BF),
            pltpu.VMEM((rows // 2, width), BF),
            pltpu.VMEM((rows // 2, width), BF),
            pltpu.VMEM((rows, width), BF),
            pltpu.VMEM((rows, width), BF),
            dma((5,)), dma((3, NZ, 2)), dma((NZ, 2)), dma((NZ, 2)), dma((NZ + 1, 2)),
            dma((3,)), dma((3,)),
            dma((4,)), dma((4,)), dma((4,)), dma((4,)),
            dma((4,)), dma((4,)), dma((4,)), dma((4,)),
            dma((3, NZ)), dma((3, NZ)),
            dma((NY,)), dma((NY,)), dma((6,)), dma((6,)),
        ],
        compiler_params=pltpu.CompilerParams(
            collective_id=0, has_side_effects=True, vmem_limit_bytes=60 * 1024 * 1024
        ),
    )(queries, keys, values, out_weight, lengths)


def solution(mesh):
    placed = (P("tok", "head"), P("tok", "head"), P("tok", "head"), P(), P("head", "tok"))
    return jax.shard_map(
        body, mesh=mesh, in_specs=placed, out_specs=P("tok", "head"), check_vma=False
    )
```

```python
import functools
import math

import jax
import jax.numpy as jnp
from jax import lax
from jax.experimental import pallas as pl
from jax.experimental.pallas import tpu as pltpu
from jax.sharding import PartitionSpec as P

HD = 128
NX, NZ, NY = 4, 8, 4
MESH = pl.DeviceIdType.MESH
FAR = -1e30
BF = jnp.bfloat16
F32 = jnp.float32
PLAN = {
    1: ((0, 1), (2, 0, 1), (2, 0, 2), (2, 1, 0)),
    2: ((0, 2), (2, 0, 3), (2, 0, 4), (2, 1, 1), (2, 1, 2), (1, 0)),
    3: ((0, 3), (2, 0, 5), (2, 1, 3), (2, 1, 4), (2, 2, 1)),
    4: ((0, 4), (2, 0, 6), (2, 1, 5), (1, 1)),
    5: ((2, 0, 7), (2, 1, 6), (2, 2, 2), (2, 2, 4), (2, 2, 5)),
    6: ((1, 2),),
    7: ((2, 1, 7), (2, 2, 0)),
    8: ((2, 2, 3), (2, 2, 6), (2, 2, 7), (1, 3)),
}


def kernel(
    scale,
    q_hbm, k_hbm, v_hbm, w_hbm, len_ref, o_ref,
    q, kv, wa, wb, start, top, total, accum, attn, mid, give, take, up, down, rup, rdown, tup, tdown,
    load, kv_recv, zp, zm, xs,
    axs, axr, azps, azpr, azms, azmr, bzps, bzpr, bzms, bzmr, bxs, bxr,
    gs, gr, rs, rr,
):
    tok = lax.axis_index("tok")
    head = lax.axis_index("head")
    x, z = lax.div(tok, NZ), lax.rem(tok, NZ)
    y, core = lax.div(head, 2), lax.rem(head, 2)
    rows = q.shape[0]
    ratio = q.shape[1] // HD
    ha = wa.shape[2]

    def at_xz(xx, zz):
        return {"tok": lax.rem(xx + NX, NX) * NZ + lax.rem(zz + NZ, NZ), "head": head}

    def at_y(yy, cc):
        return {"tok": tok, "head": lax.rem(yy + NY, NY) * 2 + cc}

    def remote(src, dst, send, recv, dev):
        return pltpu.make_async_remote_copy(
            src_ref=src, dst_ref=dst, send_sem=send, recv_sem=recv,
            device_id=dev, device_id_type=MESH,
        )

    east, west, south = at_xz(x + 1, z), at_xz(x + 3, z), at_xz(x + 2, z)
    zup, zdown = at_xz(x, z + 1), at_xz(x, z + 7)
    pair = at_y(y, 1 - core)
    yup, ydown = at_y(y + 1, core), at_y(y + 3, core)

    loads = [
        pltpu.make_async_copy(k_hbm, kv.at[0, z, 0], load.at[0]),
        pltpu.make_async_copy(v_hbm, kv.at[0, z, 1], load.at[1]),
        pltpu.make_async_copy(w_hbm.at[pl.ds(0, ha)], wa.at[z, x], load.at[2]),
        pltpu.make_async_copy(w_hbm.at[pl.ds(ha, wb.shape[2])], wb.at[x, z], load.at[3]),
        pltpu.make_async_copy(q_hbm, q, load.at[4]),
    ]
    for c in loads:
        c.start()

    barrier = pltpu.get_barrier_semaphore()
    greeted = (east, west, south, zup, zdown, pair, yup, ydown)
    for dev in greeted:
        pl.semaphore_signal(barrier, inc=1, device_id=dev, device_id_type=MESH)
    pl.semaphore_wait(barrier, len(greeted))

    def kv_zup(zz, p):
        b = kv.at[0, zz, p]
        return remote(b, b, zp.at[zz, p], kv_recv.at[0, zz, p], zup)

    def kv_zdown(zz, p):
        b = kv.at[1, zz, p]
        return remote(b, b, zm.at[zz, p], kv_recv.at[1, zz, p], zdown)

    def kv_east(t, zz, k, p):
        return remote(
            kv.at[t, zz, p], kv.at[t + 1, zz, p], xs.at[k, p], kv_recv.at[t + 1, zz, p], east
        )

    def kv_arrive(t, zz, p):
        b = kv.at[t, zz, p]
        remote(b, b, zp.at[0, p], kv_recv.at[t, zz, p], east).wait_recv()

    def item(k):
        na, nb = z + 1, NZ - z
        m = jnp.minimum(na, nb)
        both = k < 2 * m
        kind = jnp.where(both, lax.rem(k, 2), jnp.where(na > nb, 0, 1))
        j = jnp.where(both, lax.div(k, 2), k - m)
        return kind, jnp.where(kind == 0, z - j, z + j)

    def kv_first(p):
        b = kv.at[0, 0, p]
        return remote(b, b, zm.at[0, p], kv_recv.at[0, 0, p], zdown)

    def kv_last(p):
        b = kv.at[1, NZ - 1, p]
        return remote(b, b, zp.at[NZ - 1, p], kv_recv.at[1, NZ - 1, p], zup)

    def ax(d):
        return remote(wa.at[z, x], wa.at[z, x], axs.at[d - 1], axr.at[d - 1], at_xz(x + d, z))

    def azp(s):
        b = wa.at[lax.rem(z + NZ - s, NZ)]
        return remote(b, b, azps.at[s], azpr.at[s], zup)

    def azm(s):
        b = wa.at[lax.rem(z + s, NZ)]
        return remote(b, b, azms.at[s], azmr.at[s], zdown)

    def bzp(s):
        b = wb.at[x, lax.rem(z + NZ - s, NZ)]
        return remote(b, b, bzps.at[s], bzpr.at[s], zup)

    def bzm(s):
        b = wb.at[x, lax.rem(z + s, NZ)]
        return remote(b, b, bzms.at[s], bzmr.at[s], zdown)

    order = (0, 1, 7, 2, 6, 3, 5, 4)

    def bx(d, i):
        b = wb.at[lax.rem(x + d, NX), lax.rem(z + order[i], NZ)]
        return remote(b, b, bxs.at[d, i], bxr.at[d, i], west)

    last_up, last_down = lax.rem(z + 1, NZ) < 4, lax.rem(z + 7, NZ) >= 4
    get_up, get_down = z < 4, z >= 4

    def hop(up, down, s):
        if s == 4:

            @pl.when(get_up)
            def _():
                up(3).wait_recv()

            @pl.when(get_down)
            def _():
                down(3).wait_recv()

            return
        if s:
            up(s - 1).wait_recv()
            down(s - 1).wait_recv()
        if s < 3:
            up(s).start()
            down(s).start()
        else:

            @pl.when(last_up)
            def _():
                up(3).start()

            @pl.when(last_down)
            def _():
                down(3).start()

    def relay(kind, s, i=0):
        if kind == 0:
            hop(bzp, bzm, s)
        elif kind == 1:
            if s == 0:
                for d in (1, 2, 3):
                    ax(d).wait_recv()
            hop(azp, azm, s)
        else:
            if s:
                bx(s - 1, i).wait_recv()
            bx(s, i).start()

    for p in (0, 1):
        loads[p].wait()

        @pl.when(z < NZ - 1)
        def _():
            kv_zup(z, p).start()

        @pl.when(z == 0)
        def _():
            kv_first(p).start()

        @pl.when(x < NX - 1)
        def _():
            kv_east(0, z, 0, p).start()

    loads[3].wait()
    bzp(0).start()
    bzm(0).start()
    bx(0, 0).start()
    loads[2].wait()
    for d in (1, 2, 3):
        ax(d).start()
    loads[4].wait()

    qpos = tok * rows + lax.broadcasted_iota(jnp.int32, (rows, HD), 0)
    edge = jnp.int32(0)
    first = jnp.zeros((rows, HD), jnp.int32)
    for d in range(len_ref.shape[0]):
        edge = edge + len_ref[d]
        first = jnp.maximum(first, jnp.where(qpos >= edge, edge, 0))
    start[...] = first

    lane = lax.broadcasted_iota(jnp.int32, (rows, HD), 1)
    tiles = rows // HD

    def attend(t, zz, fresh):
        base = ((x - t) * NZ + zz) * rows
        kblock = kv[t, zz, 0]
        vblock = kv[t, zz, 1]
        near = start[...] - base
        allowed = []
        for j in range(tiles):
            ok = lane + j * HD >= near
            if fresh:
                ok = ok & (lane + j * HD <= lax.broadcasted_iota(jnp.int32, (rows, HD), 0))
            allowed.append(ok)
        for r in range(ratio):
            s = lax.dot_general(
                q[:, r * HD : (r + 1) * HD], kblock, (((1,), (1,)), ((), ())),
                preferred_element_type=F32,
            )
            parts = [
                jnp.where(allowed[j], s[:, j * HD : (j + 1) * HD], FAR) for j in range(tiles)
            ]
            peak = jnp.max(functools.reduce(jnp.maximum, parts), axis=1, keepdims=True)
            if fresh:
                new = jnp.broadcast_to(peak, (rows, HD))
            else:
                old = top[r]
                new = jnp.maximum(old, peak)
                fade = jnp.exp2((old - new) * scale)
            weights = [jnp.exp2((p - new) * scale) for p in parts]
            added = functools.reduce(jnp.add, weights)
            low = jnp.concatenate([w.astype(BF) for w in weights], axis=1)
            gain = jnp.dot(low, vblock, preferred_element_type=F32)
            top[r] = new
            if fresh:
                total[r] = added
                accum[r] = gain
            else:
                total[r] = total[r] * fade + added
                accum[r] = accum[r] * fade + gain

    attend(0, z, True)

    def step(k, carry):
        have_a = k <= z
        have_b = (x > 0) & (z + k - 1 < NZ) & ((z > 0) | (k < NZ))
        have_r = (x > 0) & (z == 0) & (k == 2)
        az, bz = z - k, z + k - 1

        kind, zz = item(k)
        have_item = (k <= NZ) & (x < NX - 1) & ((kind == 0) | (x > 0))
        for p in (0, 1):

            @pl.when(have_a)
            def _():
                kv_arrive(0, az, p)

            @pl.when(have_a & (z < NZ - 1) & ((z < NZ - 2) | (az > 0)))
            def _():
                kv_zup(az, p).start()

            @pl.when(have_b)
            def _():
                kv_arrive(1, bz, p)

            @pl.when(have_b & (z > 0) & ((z > 1) | (bz < NZ - 1)))
            def _():
                kv_zdown(bz, p).start()

            @pl.when((k == 1) & (x > 0) & (z == NZ - 1))
            def _():
                kv_last(p).start()

            @pl.when(have_r)
            def _():
                kv_arrive(1, NZ - 1, p)

            @pl.when(have_item)
            def _():
                kv_east(kind, zz, k, p).start()

        for when, moves in PLAN.items():

            @pl.when(k == when)
            def _():
                for move in moves:
                    relay(*move)

        @pl.when(have_a)
        def _():
            attend(0, az, False)

        @pl.when(have_b)
        def _():
            attend(1, bz, False)

        @pl.when(have_r)
        def _():
            attend(1, NZ - 1, False)

        kind, zz = item(k - 1)
        have_x = (k > 1) & (x > 0) & ((kind == 0) | (x > 1))

        @pl.when(have_x)
        def _():
            kv_arrive(kind + 1, zz, 0)
            kv_arrive(kind + 1, zz, 1)
            attend(kind + 1, zz, False)

        return carry

    lax.fori_loop(1, NZ + 2, step, 0)

    for r in range(ratio):
        whole = jnp.sum(total[r], axis=1, keepdims=True)
        attn[:, r * HD : (r + 1) * HD] = (accum[r] / whole).astype(BF)

    for i in range(NZ):
        bx(2, i).wait_recv()
    hop(azp, azm, 4)

    def project(g, c):
        out = []
        for h in (0, 2):
            zz = c * 4 + h
            left = jnp.concatenate([wa[zz, g], wb[g, zz]], axis=0)
            right = jnp.concatenate([wa[zz + 1, g], wb[g, zz + 1]], axis=0)
            both = jnp.concatenate([left, right], axis=1)
            out.append(jnp.dot(attn[...], both, preferred_element_type=F32))
        return jnp.concatenate(out, axis=1)

    def swap(i):
        return remote(give.at[i], take.at[i], gs.at[i], gr.at[i], pair)

    half = rows // 2
    lo, hi = pl.ds(0, half), pl.ds(half, half)
    targets = [lax.rem(y + d, NY) for d in (2, 1, 3, 0)]

    def first_pass(i, carry):
        g = lax.rem(y + jnp.where(i == 0, 2, jnp.where(i == 1, 1, jnp.where(i == 2, 3, 0))), NY)
        give[i] = project(g, 1 - core).astype(BF)
        swap(i).start()
        return carry

    lax.fori_loop(0, NY, first_pass, 0)

    far_up = remote(mid.at[lo], rup, rs.at[0], rr.at[0], yup)
    far_down = remote(mid.at[hi], rdown, rs.at[1], rr.at[1], ydown)
    up_hi = remote(up.at[hi], tup.at[hi], rs.at[2], rr.at[2], yup)
    down_lo = remote(down.at[lo], tdown.at[lo], rs.at[3], rr.at[3], ydown)
    up_lo = remote(up.at[lo], tup.at[lo], rs.at[4], rr.at[4], yup)
    down_hi = remote(down.at[hi], tdown.at[hi], rs.at[5], rr.at[5], ydown)

    def both_cores(i):
        mine = project(targets[i], core)
        swap(i).wait_recv()
        return mine + take[i].astype(F32)

    mid[...] = both_cores(0).astype(BF)
    far_up.start()
    far_down.start()
    part = both_cores(1)
    up[hi] = part[half:].astype(BF)
    accum_up = part[:half]
    up_hi.start()
    part = both_cores(2)
    down[lo] = part[:half].astype(BF)
    accum_down = part[half:]
    down_lo.start()
    far_up.wait_recv()
    up[lo] = (accum_up + rup[...].astype(F32)).astype(BF)
    up_lo.start()
    far_down.wait_recv()
    down[hi] = (accum_down + rdown[...].astype(F32)).astype(BF)
    down_hi.start()
    mine = both_cores(3)
    up_hi.wait_recv()
    down_lo.wait_recv()
    up_lo.wait_recv()
    down_hi.wait_recv()
    o_ref[...] = (mine + tup[...].astype(F32) + tdown[...].astype(F32)).astype(BF)

    for i in range(NY):
        swap(i).wait_send()
    for c in (far_up, far_down, up_hi, down_lo, up_lo, down_hi):
        c.wait_send()
    for d in (1, 2, 3):
        ax(d).wait_send()
    for s in range(3):
        for c in (azp(s), azm(s), bzp(s), bzm(s), *(bx(s, i) for i in range(NZ))):
            c.wait_send()

    @pl.when(last_up)
    def _():
        azp(3).wait_send()
        bzp(3).wait_send()

    @pl.when(last_down)
    def _():
        azm(3).wait_send()
        bzm(3).wait_send()

    def drain(k, carry):
        @pl.when((k <= z) & (z < NZ - 1) & ((z < NZ - 2) | (k > 0)))
        def _():
            for p in (0, 1):
                kv_zup(k, p).wait_send()

        @pl.when((k >= z) & (z > 0) & (x > 0) & (k < NZ) & ((z > 1) | (k < NZ - 1)))
        def _():
            for p in (0, 1):
                kv_zdown(k, p).wait_send()

        @pl.when((k == 0) & (z == 0))
        def _():
            for p in (0, 1):
                kv_first(p).wait_send()

        @pl.when((k == 0) & (x > 0) & (z == NZ - 1))
        def _():
            for p in (0, 1):
                kv_last(p).wait_send()

        kind, zz = item(k)

        @pl.when((x < NX - 1) & ((kind == 0) | (x > 0)))
        def _():
            kv_east(kind, zz, k, 0).wait_send()
            kv_east(kind, zz, k, 1).wait_send()

        return carry

    lax.fori_loop(0, NZ + 1, drain, 0)


def body(queries, keys, values, lengths, out_weight):
    rows, width = queries.shape
    depth = out_weight.shape[0]
    ha = depth * 11 // 32
    scale = math.log2(math.e) / math.sqrt(HD)
    ratio = width // HD
    dma = pltpu.SemaphoreType.DMA
    any_ = pl.BlockSpec(memory_space=pl.ANY)
    return pl.pallas_call(
        functools.partial(kernel, scale),
        out_shape=jax.ShapeDtypeStruct((rows, width), BF),
        in_specs=[any_, any_, any_, any_, pl.BlockSpec(memory_space=pltpu.SMEM)],
        out_specs=pl.BlockSpec(memory_space=pltpu.VMEM),
        scratch_shapes=[
            pltpu.VMEM((rows, width), BF),
            pltpu.VMEM((3, NZ, 2, rows, HD), BF),
            pltpu.VMEM((NZ, NX, ha, HD), BF),
            pltpu.VMEM((NX, NZ, depth - ha, HD), BF),
            pltpu.VMEM((rows, HD), jnp.int32),
            pltpu.VMEM((ratio, rows, HD), F32),
            pltpu.VMEM((ratio, rows, HD), F32),
            pltpu.VMEM((ratio, rows, HD), F32),
            pltpu.VMEM((rows, width), BF),
            pltpu.VMEM((rows, width), BF),
            pltpu.VMEM((NY, rows, width), BF),
            pltpu.VMEM((NY, rows, width), BF),
            pltpu.VMEM((rows, width), BF),
            pltpu.VMEM((rows, width), BF),
            pltpu.VMEM((rows // 2, width), BF),
            pltpu.VMEM((rows // 2, width), BF),
            pltpu.VMEM((rows, width), BF),
            pltpu.VMEM((rows, width), BF),
            dma((5,)), dma((3, NZ, 2)), dma((NZ, 2)), dma((NZ, 2)), dma((NZ + 1, 2)),
            dma((3,)), dma((3,)),
            dma((4,)), dma((4,)), dma((4,)), dma((4,)),
            dma((4,)), dma((4,)), dma((4,)), dma((4,)),
            dma((3, NZ)), dma((3, NZ)),
            dma((NY,)), dma((NY,)), dma((6,)), dma((6,)),
        ],
        compiler_params=pltpu.CompilerParams(
            collective_id=0, has_side_effects=True, vmem_limit_bytes=60 * 1024 * 1024
        ),
    )(queries, keys, values, out_weight, lengths)


def solution(mesh):
    placed = (P("tok", "head"), P("tok", "head"), P("tok", "head"), P(), P("head", "tok"))
    return jax.shard_map(
        body, mesh=mesh, in_specs=placed, out_specs=P("tok", "head"), check_vma=False
    )
```
